32 devices in a mesh: node: 4 (over z), chip: 8 (over y, x, core).
Axes of the slice: x: 2, y: 2, z: 4, core: 2. Of those that a mesh axis runs over, the one named last changes fastest.
Arguments:
- tokens: bfloat16 [512, 3584], P(('node', 'chip')), may hold values from -6 to 6
- expert_ids: int32 [512, 8], P(('node', 'chip')), may hold values from 0 to 31, all different within a row; in each aligned block of 16 rows (0 to 15, 16 to 31, ...) at most 8 rows name the same one
- route_weight: float32 [512, 8], P(('node', 'chip')), may hold values from 0.1 to 1
- expert_gate: bfloat16 [32, 3584, 1024], P(('node', 'chip')), may hold values from -0.09375 to 0.09375
- expert_up: bfloat16 [32, 3584, 1024], P(('node', 'chip')), may hold values from -0.09375 to 0.09375
- expert_down: bfloat16 [32, 1024, 3584], P(('node', 'chip')), may hold values from -0.1875 to 0.1875
- shared_gate: bfloat16 [3584, 2048], P(None, 'chip'), may hold values from -0.09375 to 0.09375
- shared_up: bfloat16 [3584, 2048], P(None, 'chip'), may hold values from -0.09375 to 0.09375
- shared_down: bfloat16 [2048, 3584], P('chip'), may hold values from -0.125 to 0.125
- query_latent: bfloat16 [128, 64, 512], P(('node', 'chip')), may hold values from -32 to 32
- query_rope: bfloat16 [128, 4096], P(('node', 'chip')), may hold values from -4 to 4
- cache_latent: bfloat16 [128, 128, 512], P(('node', 'chip')), may hold values from -8 to 8
- cache_rope: bfloat16 [128, 64, 128], P(('node', 'chip')), may hold values from -4 to 4
- cache_len: int32 [128], P(('node', 'chip')), may hold values from 2 to 128
Outputs:
- moe_out: bfloat16 [512, 3584], P(('node', 'chip'))
- attn_out: bfloat16 [128, 64, 512], P(('node', 'chip'))
The draws below stay inside these ranges and needn't reach their ends.
Inputs may be any that keep to these rules, and one draw needn't show every extreme that they name: `expert_ids`: a row names 8 different experts; the rows of one device name any one expert at most 8 times, a bound that some block reaches.
All inputs are finite; a program needn't handle non-finite values.
Results may differ from the reference program's by a relative error of at most 0.0085.
Values may be sent and summed in bfloat16 or wider, within the bound.
A program may use at most 128 MiB of HBM per device.

```python
import math
import jax
import jax.numpy as jnp
import numpy as np
from jax import lax

D = 3584
FF = 1024
FFS = 2048
TOPK = 8
HEADS = 64
LATENT = 512
ROPE = 64
TOK_DEV = 16
CACHE = 128
EXPERTS = 32
CAP = 8
TOKENS = 512
ALL_SEQS = 128
N_NODE = 4
N_CHIP = 8


def latent_fields(key):
    key_list = jax.random.split(jax.random.fold_in(key, 7), 3)
    cache_vals = jnp.clip(jax.random.normal(key_list[0], (ALL_SEQS, CACHE, LATENT), jnp.float32), -4.0, 4.0)
    queries = jnp.clip(jax.random.normal(key_list[1], (ALL_SEQS, HEADS, LATENT), jnp.float32), -4.0, 4.0)
    rope_vals = jnp.clip(jax.random.normal(key_list[2], (ALL_SEQS, HEADS * ROPE), jnp.float32), -4.0, 4.0)
    return (queries, rope_vals, cache_vals)


def draw_query_latent(key, part):
    return latent_fields(key)[0].astype(jnp.bfloat16)


def draw_query_rope(key, part):
    return latent_fields(key)[1].astype(jnp.bfloat16)


def draw_cache_latent(key, part):
    return latent_fields(key)[2].astype(jnp.bfloat16)


def touch_ends(entries, stream_key, least, high):
    shape = entries.shape
    index_at = [jax.random.randint(jax.random.fold_in(stream_key, axis), (), 0, shape[axis]) for axis in range(len(shape))]
    entries = entries.at[tuple(index_at)].set(least)
    longest = shape.index(max(shape))
    index_at[longest] = (index_at[longest] + 1) % shape[longest]
    return entries.at[tuple(index_at)].set(high)


def shard_levels(own_key, shape, cuts, least, high):
    gain, own = 1.0, jax.random.fold_in(own_key, 6)
    for dim, parts in cuts:
        heights = jnp.exp(jax.random.uniform(jax.random.fold_in(own, dim), (parts,), jnp.float32, least / len(cuts), high / len(cuts)))
        gain = gain * jnp.repeat(heights, shape[dim] // parts).reshape([-1 if axis == dim else 1 for axis in range(len(shape))])
    return gain


def deal_out(stream_key, own, number, rows, count, top, limit, skew):
    ranking = jax.random.permutation(stream_key, count)
    packed, common = shares(count, rows * top, limit, skew, True), shares(count, rows * top, limit, skew, False)
    places = jnp.arange(count)

    def named(lengths, turn):
        used = int((lengths > 0).sum())
        fixed = max(1, used // 4)
        passed = fixed + (places - fixed + turn * (used - fixed)) % max(1, count - fixed)
        return jnp.zeros((count,), jnp.int32).at[ranking[jnp.where(places < fixed, places, passed)]].set(jnp.asarray(lengths, jnp.int32))

    lengths = jnp.where(number % 4 == 0, named(packed, number // 4), named(common, number - number // 4 - 1))
    mixed = jax.random.permutation(jax.random.fold_in(own, 3), count)
    source_of, sink = mixed[0:count // 2 * 2:2], mixed[1:count // 2 * 2:2]
    room = jnp.minimum(lengths[source_of] - 1, limit - lengths[sink]) // 2
    room = jnp.where((source_of == ranking[0]) | (sink == ranking[0]) | (lengths[sink] == 0), 0, jnp.maximum(room, 0))
    passed = jax.random.randint(jax.random.fold_in(own, 4), (count // 2,), 0, 1 << 20) % (room + 1)
    lengths = lengths.at[source_of].add(-passed).at[sink].add(passed)
    members = jnp.searchsorted(jnp.cumsum(lengths), jnp.arange(rows * top), side="right").astype(jnp.int32)
    grid = members.reshape(top, rows).T
    grid = grid[jax.random.permutation(jax.random.fold_in(own, 1), rows)]
    turn = jax.random.randint(jax.random.fold_in(own, 2), (rows, 1), 0, top)
    return jnp.take_along_axis(grid, (jnp.arange(top)[None, :] + turn) % top, axis=1)


def shares(count, total, bound, slope, full):
    portions = [(1 << 20) // math.isqrt(grade ** slope) + 1 for grade in range(1, count + 1)]
    largest = bound if full else min(bound, max(-(-total // count), total * portions[0] // sum(portions)))
    least = 1 if total - largest >= count - 1 else 0
    given, spare = [largest] + [least] * (count - 1), total - largest - least * (count - 1)
    while spare > 0:
        free = [i for i in range(1, count) if given[i] < largest] or [i for i in range(1, count) if given[i] < bound]
        whole, budget = sum([portions[i] for i in free]), spare
        for i in free:
            extra = min(bound - given[i], max(1, budget * portions[i] // whole), spare)
            given[i] = given[i] + extra
            spare = spare - extra
    return np.array(given)


def noise(stream_key, extent, scale, limit, shards=(), kind=jnp.bfloat16):
    level = shard_levels(stream_key, extent, shards, -0.22, 0.18) if shards else 1.0
    entries = jax.random.normal(stream_key, extent, jnp.float32) * scale * level
    return jnp.minimum(jnp.maximum(entries, -limit), limit).astype(kind)


def setup_inputs(seed: int = 0) -> dict:
    keys = jax.random.split(jax.random.key(seed), 15)
    tokens = noise(keys[0], (TOKENS, D), 1.0, 6.0, ((0, 32),))
    expert_ids_keys = jax.random.split(jax.random.fold_in(keys[1], 1), TOKENS // TOK_DEV)
    expert_ids_turns = jax.random.permutation(jax.random.fold_in(keys[1], 3), TOKENS // TOK_DEV)
    expert_ids = jax.vmap(lambda own, number: deal_out(jax.random.fold_in(keys[1], 2), own, number, TOK_DEV, EXPERTS, TOPK, CAP, 2))(expert_ids_keys, expert_ids_turns).reshape((TOKENS, TOPK))
    route_weight = jnp.clip(jnp.exp(math.log(1.0) - 2.3025851 * jax.random.uniform(keys[2], (TOKENS, TOPK), jnp.float32) ** shard_levels(keys[2], (TOKENS, TOPK), ((0, 32),), -0.2, 0.2)), 0.1, 1.0)
    expert_gate = noise(keys[3], (EXPERTS, D, FF), D ** -0.5, 0.09375, ((0, 32),))
    expert_up = noise(keys[4], (EXPERTS, D, FF), D ** -0.5, 0.09375, ((0, 32),))
    expert_down = noise(keys[5], (EXPERTS, FF, D), FF ** -0.5, 0.1875, ((0, 32),))
    shared_gate = noise(keys[6], (D, FFS), D ** -0.5, 0.09375, ((1, 8),))
    shared_up = noise(keys[7], (D, FFS), D ** -0.5, 0.09375, ((1, 8),))
    shared_down = noise(keys[8], (FFS, D), FFS ** -0.5, 0.125, ((0, 8),))
    query_latent = draw_query_latent(jax.random.fold_in(keys[14], 71), 0)
    query_rope = draw_query_rope(jax.random.fold_in(keys[14], 71), 0)
    cache_latent = draw_cache_latent(jax.random.fold_in(keys[14], 71), 0)
    cache_rope = noise(keys[12], (ALL_SEQS, ROPE, CACHE), 1.0, 4.0, ((0, 32),))
    cache_len = touch_ends(jax.random.randint(keys[13], (ALL_SEQS,), 2, CACHE + 1), jax.random.fold_in(keys[13], 1), 2, CACHE).astype(jnp.int32)
    return dict(tokens=tokens, expert_ids=expert_ids, route_weight=route_weight, expert_gate=expert_gate, expert_up=expert_up, expert_down=expert_down, shared_gate=shared_gate, shared_up=shared_up, shared_down=shared_down, query_latent=query_latent, query_rope=query_rope, cache_latent=cache_latent, cache_rope=cache_rope, cache_len=cache_len)


score_scale = 192.0 ** -0.5


def swiglu_hidden(token_rows, gate_matrix, up_matrix):
    gate_part = jnp.dot(token_rows, gate_matrix, preferred_element_type=jnp.float32)
    up_part = jnp.dot(token_rows, up_matrix, preferred_element_type=jnp.float32)
    return (jax.nn.silu(gate_part) * up_part).astype(jnp.bfloat16)


def attend(query_latent, query_rope, cache_latent, cache_rope, cache_len):
    seq_count, head_count, latent_width = query_latent.shape
    rope_width = cache_rope.shape[1]
    cache_size = cache_rope.shape[2]
    rope_query = query_rope.reshape(seq_count, head_count, rope_width).astype(jnp.float32)
    cache_float = cache_latent.astype(jnp.float32)
    scores = jnp.einsum("shl,spl->shp", query_latent.astype(jnp.float32), cache_float)
    scores = scores + jnp.einsum("shr,srp->shp", rope_query, cache_rope.astype(jnp.float32))
    scores = scores * score_scale
    position = jnp.arange(cache_size, dtype=jnp.int32)
    live_mask = position[None, None, :] < cache_len[:, None, None]
    masked = jnp.where(live_mask, scores, -1e30)
    row_peak = jnp.max(masked, axis=2, keepdims=True)
    weight = jnp.where(live_mask, jnp.exp(masked - row_peak), 0.0)
    softmax_weight = (weight / jnp.sum(weight, axis=2, keepdims=True)).astype(jnp.bfloat16)
    attended = jnp.einsum("shp,spl->shl", softmax_weight.astype(jnp.float32), cache_float)
    return attended.astype(jnp.bfloat16)


def reference(tokens, expert_ids, route_weight, expert_gate, expert_up, expert_down, shared_gate, shared_up, shared_down, query_latent, query_rope, cache_latent, cache_rope, cache_len):
    experts = N_NODE * N_CHIP
    devices = experts
    model_width = tokens.shape[1]
    per_device = TOK_DEV * TOPK
    flat_ids = expert_ids.reshape(devices, per_device).astype(jnp.int32)
    onehot = (flat_ids[:, :, None] == jnp.arange(experts, dtype=jnp.int32)[None, None, :]).astype(jnp.int32)
    earlier = jnp.cumsum(onehot, axis=1) - onehot
    slot_index = jnp.sum(earlier * onehot, axis=2).astype(jnp.int32)
    source = jnp.broadcast_to(jnp.arange(devices, dtype=jnp.int32)[:, None], (devices, per_device))
    assign = jnp.arange(devices * per_device, dtype=jnp.int32).reshape(devices, per_device)
    slot_table = jnp.full((experts, devices, CAP), -1, jnp.int32).at[flat_ids, source, slot_index].set(assign)
    weights_flat = route_weight.reshape(-1)

    def one_expert(totals, expert_index):
        owner_slots = slot_table[expert_index].reshape(-1)
        live_slot = owner_slots >= 0
        safe_index = jnp.where(live_slot, owner_slots, 0).astype(jnp.int32)
        token_index = (safe_index // TOPK).astype(jnp.int32)
        hidden = swiglu_hidden(tokens[token_index], expert_gate[expert_index], expert_up[expert_index])
        result = jnp.dot(hidden, expert_down[expert_index], preferred_element_type=jnp.float32).astype(jnp.bfloat16)
        scale_row = jnp.where(live_slot, weights_flat[safe_index], jnp.zeros((), jnp.float32))
        totals = totals.at[token_index].add(scale_row[:, None] * result.astype(jnp.float32))
        return totals, None

    routed, _ = lax.scan(one_expert, jnp.zeros((tokens.shape[0], model_width), jnp.float32), jnp.arange(experts, dtype=jnp.int32))
    shared_hidden = swiglu_hidden(tokens, shared_gate, shared_up)
    shared_out = jnp.dot(shared_hidden, shared_down, preferred_element_type=jnp.float32)
    moe_out = (shared_out + routed).astype(jnp.bfloat16)
    attn_out = attend(query_latent, query_rope, cache_latent, cache_rope, cache_len)
    return (moe_out, attn_out)
```

```python
import jax
import jax.numpy as jnp
from jax import lax
from jax.experimental import pallas as pl
from jax.experimental.pallas import tpu as pltpu
from jax.sharding import PartitionSpec as P

MESH = pl.DeviceIdType.MESH
LANES = 128


score_scale = 192.0 ** (-0.5)


def swiglu_hidden(token_rows, gate_matrix, up_matrix):
    gate_part = jnp.dot(token_rows, gate_matrix, preferred_element_type=jnp.float32)
    up_part = jnp.dot(token_rows, up_matrix, preferred_element_type=jnp.float32)
    return (jax.nn.silu(gate_part) * up_part).astype(jnp.bfloat16)


def attend(query_latent, query_rope, cache_latent, cache_rope, cache_len):
    seq_count, head_count, latent_width = query_latent.shape
    rope_width = cache_rope.shape[1]
    cache_size = cache_rope.shape[2]
    rope_query = query_rope.reshape(seq_count, head_count, rope_width)
    scores = jnp.einsum(
        "shl,spl->shp", query_latent, cache_latent, preferred_element_type=jnp.float32
    )
    scores = scores + jnp.einsum(
        "shr,srp->shp", rope_query, cache_rope, preferred_element_type=jnp.float32
    )
    scores = scores * score_scale
    position = jnp.arange(cache_size, dtype=jnp.int32)
    live_mask = position[None, None, :] < cache_len[:, None, None]
    masked = jnp.where(live_mask, scores, -1e30)
    row_peak = jnp.max(masked, axis=2, keepdims=True)
    weight = jnp.where(live_mask, jnp.exp(masked - row_peak), 0.0)
    softmax_weight = (weight / jnp.sum(weight, axis=2, keepdims=True)).astype(jnp.bfloat16)
    attended = jnp.einsum(
        "shp,spl->shl", softmax_weight, cache_latent, preferred_element_type=jnp.float32
    )
    return attended.astype(jnp.bfloat16)


class Place:
    def __init__(self, nodes):
        self.nodes = nodes
        self.z = lax.axis_index("node")
        chip = lax.axis_index("chip")
        self.y, self.x, self.c = chip // 4, (chip // 2) % 2, chip % 2

    def block(self, z, y, x, c):
        return z * 8 + y * 4 + x * 2 + c

    def dev(self, z=None, y=None, x=None, c=None):
        pick = lambda new, own: own if new is None else new
        chip = pick(y, self.y) * 4 + pick(x, self.x) * 2 + pick(c, self.c)
        return {"node": pick(z, self.z), "chip": chip}

    def other_z(self, step):
        return lax.rem(self.z + step, self.nodes)

    def partners(self):
        found = [self.dev(z=self.other_z(s)) for s in range(1, self.nodes)]
        return found + [self.dev(y=1 - self.y), self.dev(x=1 - self.x), self.dev(c=1 - self.c)]


def greet(place):
    barrier = pltpu.get_barrier_semaphore()
    partners = place.partners()
    for who in partners:
        pl.semaphore_signal(barrier, inc=1, device_id=who, device_id_type=MESH)
    pl.semaphore_wait(barrier, len(partners))


def gather_kernel(nodes, own_ref, out_ref, held, z_send, z_recv, xy_send, xy_recv, c_send, c_recv,
                  own_sem, out_sem):
    p = Place(nodes)
    width = held.shape[2]
    half = width // LANES // 2 * LANES
    cols = (pl.ds(0, half), pl.ds(half, width - half))
    me = p.block(p.z, p.y, p.x, p.c)
    load = pltpu.make_async_copy(own_ref, held.at[me], own_sem)
    load.start()
    greet(p)
    load.wait()
    sends, outs = [], []

    def copy(block, h, send, recv, who):
        return pltpu.make_async_remote_copy(
            held.at[block, :, cols[h]], held.at[block, :, cols[h]], send, recv,
            device_id=who, device_id_type=MESH)

    def push(block, h, send, recv, who):
        one = copy(block, h, send, recv, who)
        one.start()
        sends.append(one)

    def arrive(block, h, sem):
        copy(block, h, sem, sem, p.dev(c=1 - p.c)).wait_recv()

    def keep(block, h):
        n = len(outs)
        one = pltpu.make_async_copy(
            held.at[block, :, cols[h]], out_ref.at[block, :, cols[h]], out_sem.at[n])
        one.start()
        outs.append(one)

    def near(h):
        return (p.dev(x=1 - p.x), p.dev(y=1 - p.y))[h]

    def far(h):
        return (p.dev(y=1 - p.y), p.dev(x=1 - p.x))[h]

    def far_source(h, z, k):
        if h == 0:
            return p.block(z, 1 - p.y, (p.x, 1 - p.x)[k], p.c)
        return p.block(z, (p.y, 1 - p.y)[k], 1 - p.x, p.c)

    def near_source(h, z):
        return p.block(z, p.y, 1 - p.x, p.c) if h == 0 else p.block(z, 1 - p.y, p.x, p.c)

    def to_core(block, h, n):
        push(block, h, c_send.at[h, n], c_recv.at[h, n], p.dev(c=1 - p.c))
        keep(block, h)

    order = [0] + [s for pair in zip(range(1, nodes), range(nodes - 1, 0, -1)) for s in pair]
    order = list(dict.fromkeys(order))
    for s in order[1:]:
        for h in range(2):
            push(me, h, z_send.at[h, s], z_recv.at[h, s], p.dev(z=p.other_z(s)))
    for s in order:
        z_from = lax.rem(p.z + nodes - s, nodes)
        block = p.block(z_from, p.y, p.x, p.c)
        for h in range(2):
            if s:
                arrive(block, h, z_recv.at[h, s])
            push(block, h, xy_send.at[h, 0, s], xy_recv.at[h, 0, s], near(h))
            push(block, h, xy_send.at[h, 1, s], xy_recv.at[h, 1, s], far(h))
            to_core(block, h, s)
    for s in order:
        z_from = lax.rem(p.z + nodes - s, nodes)
        for h in range(2):
            block = near_source(h, z_from)
            arrive(block, h, xy_recv.at[h, 0, s])
            push(block, h, xy_send.at[h, 2, s], xy_recv.at[h, 2, s], far(h))
            to_core(block, h, nodes + s)
        for h in range(2):
            block = far_source(h, z_from, 0)
            arrive(block, h, xy_recv.at[h, 1, s])
            to_core(block, h, 2 * nodes + s)
    for s in order:
        z_from = lax.rem(p.z + nodes - s, nodes)
        for h in range(2):
            block = far_source(h, z_from, 1)
            arrive(block, h, xy_recv.at[h, 2, s])
            to_core(block, h, 3 * nodes + s)
    for s in order:
        z_from = lax.rem(p.z + nodes - s, nodes)
        for h in range(2):
            core = lambda y, x: p.block(z_from, y, x, 1 - p.c)
            near_at = (p.y, 1 - p.x) if h == 0 else (1 - p.y, p.x)
            far_at = (1 - p.y, p.x) if h == 0 else (p.y, 1 - p.x)
            spots = ((p.y, p.x), near_at, far_at, (1 - p.y, 1 - p.x))
            for k, (y, x) in enumerate(spots):
                block = core(y, x)
                arrive(block, h, c_recv.at[h, k * nodes + s])
                keep(block, h)
    for one in sends:
        one.wait_send()
    for one in outs:
        one.wait()


def gather_tokens(rows, nodes):
    count, width = rows.shape
    devices = nodes * 8
    dma = pltpu.SemaphoreType.DMA
    return pl.pallas_call(
        lambda *refs: gather_kernel(nodes, *refs),
        out_shape=jax.ShapeDtypeStruct((devices, count, width), rows.dtype),
        in_specs=[pl.BlockSpec(memory_space=pl.ANY)],
        out_specs=pl.BlockSpec(memory_space=pl.ANY),
        scratch_shapes=[
            pltpu.VMEM((devices, count, width), rows.dtype),
            dma((2, nodes)), dma((2, nodes)),
            dma((2, 3, nodes)), dma((2, 3, nodes)),
            dma((2, 4 * nodes)), dma((2, 4 * nodes)),
            dma, dma((2 * devices,)),
        ],
        compiler_params=pltpu.CompilerParams(collective_id=0, has_side_effects=True),
        name="gather_tokens",
    )(rows)


def scatter_kernel(nodes, in_ref, out_ref, mine, r1, r2, r3, r4, s1, t1, s2, t2, s3, t3, s4, t4,
                   in_sem):
    p = Place(nodes)
    width = mine.shape[2]
    half = width // LANES // 2 * LANES
    cols = (pl.ds(0, half), pl.ds(half, width - half))
    loads = []
    order = list(range(1, nodes)) + [0]
    spots = {0: ((1, 1), (1, 0), (0, 1), (0, 0)), 1: ((1, 1), (0, 1), (1, 0), (0, 0))}
    sequence = [(h, k, s) for k in range(4) for s in order for h in range(2)]

    def at(h, k, s, c):
        fy, fx = spots[h][k]
        y = 1 - p.y if fy else p.y
        x = 1 - p.x if fx else p.x
        return p.block(p.other_z(s), y, x, c)

    for n, (h, k, s) in enumerate(sequence):
        for own in range(2):
            block = at(h, k, s, p.c if own else 1 - p.c)
            load = pltpu.make_async_copy(
                in_ref.at[block, :, cols[h]], mine.at[block, :, cols[h]], in_sem.at[own, n])
            load.start()
            loads.append(load)
    greet(p)
    sends = []

    def push(src, dst, send, recv, who):
        one = pltpu.make_async_remote_copy(src, dst, send, recv, device_id=who, device_id_type=MESH)
        one.start()
        sends.append(one)

    def arrive(dst, recv):
        pltpu.make_async_remote_copy(
            dst, dst, recv, recv, device_id=p.dev(c=1 - p.c), device_id_type=MESH).wait_recv()

    def plus(first, second):
        return first.astype(jnp.float32) + second.astype(jnp.float32)

    first_link = (p.dev(y=1 - p.y), p.dev(x=1 - p.x))
    second_link = (p.dev(x=1 - p.x), p.dev(y=1 - p.y))
    for n, (h, k, s) in enumerate(sequence):
        loads[2 * n].wait()
        push(mine.at[at(h, k, s, 1 - p.c), :, cols[h]], r1.at[h, k, s], s1.at[h, k, s],
             t1.at[h, k, s], p.dev(c=1 - p.c))
    for n, (h, k, s) in enumerate(sequence):
        loads[2 * n + 1].wait()
        arrive(r1.at[h, k, s], t1.at[h, k, s])
        r1[h, k, s] = plus(r1[h, k, s], mine[at(h, k, s, p.c), :, cols[h]]).astype(jnp.bfloat16)
        if k < 2:
            push(r1.at[h, k, s], r2.at[h, k, s], s2.at[h, k, s], t2.at[h, k, s], first_link[h])
    for s in order:
        for h in range(2):
            arrive(r2.at[h, 0, s], t2.at[h, 0, s])
            r2[h, 0, s] = plus(r2[h, 0, s], r1[h, 2, s]).astype(jnp.bfloat16)
            push(r2.at[h, 0, s], r3.at[h, s], s3.at[h, s], t3.at[h, s], second_link[h])
    for s in order:
        for h in range(2):
            arrive(r2.at[h, 1, s], t2.at[h, 1, s])
            arrive(r3.at[h, s], t3.at[h, s])
            total = plus(r2[h, 1, s], r1[h, 3, s]) + r3[h, s].astype(jnp.float32)
            r3[h, s] = total.astype(jnp.bfloat16)
            if s:
                push(r3.at[h, s], r4.at[h, s], s4.at[h, s], t4.at[h, s], p.dev(z=p.other_z(s)))
    for h in range(2):
        total = r3[h, 0].astype(jnp.float32)
        for s in range(1, nodes):
            arrive(r4.at[h, s], t4.at[h, s])
            total = total + r4[h, s].astype(jnp.float32)
        out_ref[:, cols[h]] = total.astype(jnp.bfloat16)
    for one in sends:
        one.wait_send()


def scatter_sums(terms, nodes):
    devices, count, width = terms.shape
    half = width // 2
    dma = pltpu.SemaphoreType.DMA
    vmem = lambda *lead: pltpu.VMEM((*lead, count, half), terms.dtype)
    return pl.pallas_call(
        lambda *refs: scatter_kernel(nodes, *refs),
        out_shape=jax.ShapeDtypeStruct((count, width), terms.dtype),
        in_specs=[pl.BlockSpec(memory_space=pl.ANY)],
        out_specs=pl.BlockSpec(memory_space=pltpu.VMEM),
        scratch_shapes=[
            pltpu.VMEM((devices, count, width), terms.dtype),
            vmem(2, 4, nodes), vmem(2, 2, nodes), vmem(2, nodes), vmem(2, nodes),
            dma((2, 4, nodes)), dma((2, 4, nodes)),
            dma((2, 2, nodes)), dma((2, 2, nodes)),
            dma((2, nodes)), dma((2, nodes)),
            dma((2, nodes)), dma((2, nodes)),
            dma((2, devices)),
        ],
        compiler_params=pltpu.CompilerParams(collective_id=1, has_side_effects=True),
        name="scatter_sums",
    )(terms)


def local(
    tokens,
    expert_ids,
    route_weight,
    expert_gate,
    expert_up,
    expert_down,
    shared_gate,
    shared_up,
    shared_down,
    query_latent,
    query_rope,
    cache_latent,
    cache_rope,
    cache_len,
):
    node_count = lax.axis_size("node")
    chip_count = lax.axis_size("chip")
    experts = node_count * chip_count
    tok_rows, model_width = tokens.shape
    top = expert_ids.shape[1]
    slots = (2 * tok_rows * top + experts - 1) // experts
    trees = chip_count == 8
    node, chip = lax.axis_index("node"), lax.axis_index("chip")
    me = node * chip_count + chip

    names = jnp.arange(experts, dtype=jnp.int32)
    dense = jnp.sum(
        jnp.where(expert_ids[:, :, None] == names, route_weight[:, :, None], 0.0), axis=1
    )
    high = lax.reduce_precision(dense, 8, 7)
    low = dense - high
    side = jnp.concatenate([high, low], axis=1).astype(jnp.bfloat16)
    side = jnp.pad(side, ((0, 0), (0, -(2 * experts) % LANES)))
    rows = jnp.concatenate([tokens, side], axis=1)
    if trees:
        gathered = gather_tokens(rows, node_count)
    else:
        gathered = lax.all_gather(rows, ("node", "chip"), axis=0)
    total = experts * tok_rows
    flat = gathered.reshape(total, -1)
    every = flat[:, :model_width]
    tail = flat[:, model_width:].astype(jnp.float32)
    lane = lax.broadcasted_iota(jnp.int32, (1, tail.shape[1]), 1)
    scale = jnp.sum(jnp.where((lane == me) | (lane == experts + me), tail, 0.0), axis=1)

    chosen = (scale > 0).reshape(experts, tok_rows)
    rank = jnp.cumsum(chosen.astype(jnp.int32), axis=1) - 1
    slot = jnp.where(chosen, rank + slots * names[:, None], -1).reshape(-1)
    place = (jnp.arange(experts * slots, dtype=jnp.int32)[:, None] == slot[None, :])
    place = place.astype(jnp.bfloat16)
    picked = jnp.dot(place, every, preferred_element_type=jnp.float32).astype(jnp.bfloat16)
    hidden = swiglu_hidden(picked, expert_gate[0], expert_up[0])
    result = jnp.dot(hidden, expert_down[0], preferred_element_type=jnp.float32)
    result = result.astype(jnp.bfloat16)
    spread = lax.dot_general(
        place, result, (((0,), (0,)), ((), ())), preferred_element_type=jnp.float32
    )
    group = lax.dynamic_slice_in_dim(every, node * chip_count * tok_rows, chip_count * tok_rows, 0)
    shared_hidden = swiglu_hidden(group, shared_gate, shared_up)
    partial_terms = jnp.dot(shared_hidden, shared_down, preferred_element_type=jnp.float32)
    in_group = (names // chip_count == node).astype(jnp.float32)
    terms = (spread * scale[:, None]).reshape(node_count, -1, model_width)
    own_node = jnp.arange(node_count) == node
    terms = terms + jnp.where(own_node[:, None, None], partial_terms[None], 0.0)
    terms = terms.astype(jnp.bfloat16).reshape(experts, tok_rows, model_width)
    if trees:
        moe_out = scatter_sums(terms, node_count)
    else:
        moe_out = lax.psum_scatter(
            terms.reshape(total, model_width), ("node", "chip"), scatter_dimension=0, tiled=True
        )
    attn_out = attend(query_latent, query_rope, cache_latent, cache_rope, cache_len)
    return (moe_out, attn_out)


def solution(mesh):
    placed = (
        P(("node", "chip"), None),
        P(("node", "chip"), None),
        P(("node", "chip"), None),
        P(("node", "chip"), None, None),
        P(("node", "chip"), None, None),
        P(("node", "chip"), None, None),
        P(None, "chip"),
        P(None, "chip"),
        P("chip", None),
        P(("node", "chip"), None, None),
        P(("node", "chip"), None),
        P(("node", "chip"), None, None),
        P(("node", "chip"), None, None),
        P(("node", "chip")),
    )
    return jax.shard_map(
        local,
        mesh=mesh,
        in_specs=placed,
        out_specs=(P(("node", "chip"), None), P(("node", "chip"), None, None)),
        check_vma=False,
    )
```

```python
import jax
import jax.numpy as jnp
from jax import lax
from jax.experimental import pallas as pl
from jax.experimental.pallas import tpu as pltpu
from jax.sharding import PartitionSpec as P

MESH = pl.DeviceIdType.MESH
LANES = 128


score_scale = 192.0 ** (-0.5)


def swiglu_hidden(token_rows, gate_matrix, up_matrix):
    gate_part = jnp.dot(token_rows, gate_matrix, preferred_element_type=jnp.float32)
    up_part = jnp.dot(token_rows, up_matrix, preferred_element_type=jnp.float32)
    return (jax.nn.silu(gate_part) * up_part).astype(jnp.bfloat16)


def attend(query_latent, query_rope, cache_latent, cache_rope, cache_len):
    seq_count, head_count, latent_width = query_latent.shape
    rope_width = cache_rope.shape[1]
    cache_size = cache_rope.shape[2]
    rope_query = query_rope.reshape(seq_count, head_count, rope_width)
    scores = jnp.einsum(
        "shl,spl->shp", query_latent, cache_latent, preferred_element_type=jnp.float32
    )
    scores = scores + jnp.einsum(
        "shr,srp->shp", rope_query, cache_rope, preferred_element_type=jnp.float32
    )
    scores = scores * score_scale
    position = jnp.arange(cache_size, dtype=jnp.int32)
    live_mask = position[None, None, :] < cache_len[:, None, None]
    masked = jnp.where(live_mask, scores, -1e30)
    row_peak = jnp.max(masked, axis=2, keepdims=True)
    weight = jnp.where(live_mask, jnp.exp(masked - row_peak), 0.0)
    softmax_weight = (weight / jnp.sum(weight, axis=2, keepdims=True)).astype(jnp.bfloat16)
    attended = jnp.einsum(
        "shp,spl->shl", softmax_weight, cache_latent, preferred_element_type=jnp.float32
    )
    return attended.astype(jnp.bfloat16)


class Place:
    def __init__(self, nodes):
        self.nodes = nodes
        self.z = lax.axis_index("node")
        chip = lax.axis_index("chip")
        self.y, self.x, self.c = chip // 4, (chip // 2) % 2, chip % 2

    def block(self, z, y, x, c):
        return z * 8 + y * 4 + x * 2 + c

    def dev(self, z=None, y=None, x=None, c=None):
        pick = lambda new, own: own if new is None else new
        chip = pick(y, self.y) * 4 + pick(x, self.x) * 2 + pick(c, self.c)
        return {"node": pick(z, self.z), "chip": chip}

    def other_z(self, step):
        return lax.rem(self.z + step, self.nodes)

    def partners(self):
        found = [self.dev(z=self.other_z(s)) for s in range(1, self.nodes)]
        return found + [self.dev(y=1 - self.y), self.dev(x=1 - self.x), self.dev(c=1 - self.c)]


def greet(place):
    barrier = pltpu.get_barrier_semaphore()
    partners = place.partners()
    for who in partners:
        pl.semaphore_signal(barrier, inc=1, device_id=who, device_id_type=MESH)
    pl.semaphore_wait(barrier, len(partners))


def gather_kernel(nodes, own_ref, out_ref, held, z_send, z_recv, xy_send, xy_recv, c_send, c_recv,
                  own_sem, out_sem):
    p = Place(nodes)
    width = held.shape[2]
    half = width // LANES // 2 * LANES
    cols = (pl.ds(0, half), pl.ds(half, width - half))
    me = p.block(p.z, p.y, p.x, p.c)
    load = pltpu.make_async_copy(own_ref, held.at[me], own_sem)
    load.start()
    greet(p)
    load.wait()
    sends, outs = [], []

    def copy(block, h, send, recv, who):
        return pltpu.make_async_remote_copy(
            held.at[block, :, cols[h]], held.at[block, :, cols[h]], send, recv,
            device_id=who, device_id_type=MESH)

    def push(block, h, send, recv, who):
        one = copy(block, h, send, recv, who)
        one.start()
        sends.append(one)

    def arrive(block, h, sem):
        copy(block, h, sem, sem, p.dev(c=1 - p.c)).wait_recv()

    def keep(block, h):
        n = len(outs)
        one = pltpu.make_async_copy(
            held.at[block, :, cols[h]], out_ref.at[block, :, cols[h]], out_sem.at[n])
        one.start()
        outs.append(one)

    def near(h):
        return (p.dev(x=1 - p.x), p.dev(y=1 - p.y))[h]

    def far(h):
        return (p.dev(y=1 - p.y), p.dev(x=1 - p.x))[h]

    def far_source(h, z, k):
        if h == 0:
            return p.block(z, 1 - p.y, (p.x, 1 - p.x)[k], p.c)
        return p.block(z, (p.y, 1 - p.y)[k], 1 - p.x, p.c)

    def near_source(h, z):
        return p.block(z, p.y, 1 - p.x, p.c) if h == 0 else p.block(z, 1 - p.y, p.x, p.c)

    def to_core(block, h, n):
        push(block, h, c_send.at[h, n], c_recv.at[h, n], p.dev(c=1 - p.c))
        keep(block, h)

    order = [0] + [s for pair in zip(range(1, nodes), range(nodes - 1, 0, -1)) for s in pair]
    order = list(dict.fromkeys(order))
    for s in order[1:]:
        for h in range(2):
            push(me, h, z_send.at[h, s], z_recv.at[h, s], p.dev(z=p.other_z(s)))
    for s in order:
        z_from = lax.rem(p.z + nodes - s, nodes)
        block = p.block(z_from, p.y, p.x, p.c)
        for h in range(2):
            if s:
                arrive(block, h, z_recv.at[h, s])
            push(block, h, xy_send.at[h, 0, s], xy_recv.at[h, 0, s], near(h))
            push(block, h, xy_send.at[h, 1, s], xy_recv.at[h, 1, s], far(h))
            to_core(block, h, s)
    for s in order:
        z_from = lax.rem(p.z + nodes - s, nodes)
        for h in range(2):
            block = near_source(h, z_from)
            arrive(block, h, xy_recv.at[h, 0, s])
            push(block, h, xy_send.at[h, 2, s], xy_recv.at[h, 2, s], far(h))
            to_core(block, h, nodes + s)
        for h in range(2):
            block = far_source(h, z_from, 0)
            arrive(block, h, xy_recv.at[h, 1, s])
            to_core(block, h, 2 * nodes + s)
    for s in order:
        z_from = lax.rem(p.z + nodes - s, nodes)
        for h in range(2):
            block = far_source(h, z_from, 1)
            arrive(block, h, xy_recv.at[h, 2, s])
            to_core(block, h, 3 * nodes + s)
    for s in order:
        z_from = lax.rem(p.z + nodes - s, nodes)
        for h in range(2):
            core = lambda y, x: p.block(z_from, y, x, 1 - p.c)
            near_at = (p.y, 1 - p.x) if h == 0 else (1 - p.y, p.x)
            far_at = (1 - p.y, p.x) if h == 0 else (p.y, 1 - p.x)
            spots = ((p.y, p.x), near_at, far_at, (1 - p.y, 1 - p.x))
            for k, (y, x) in enumerate(spots):
                block = core(y, x)
                arrive(block, h, c_recv.at[h, k * nodes + s])
                keep(block, h)
    for one in sends:
        one.wait_send()
    for one in outs:
        one.wait()


def gather_tokens(rows, nodes):
    count, width = rows.shape
    devices = nodes * 8
    dma = pltpu.SemaphoreType.DMA
    return pl.pallas_call(
        lambda *refs: gather_kernel(nodes, *refs),
        out_shape=jax.ShapeDtypeStruct((devices, count, width), rows.dtype),
        in_specs=[pl.BlockSpec(memory_space=pl.ANY)],
        out_specs=pl.BlockSpec(memory_space=pl.ANY),
        scratch_shapes=[
            pltpu.VMEM((devices, count, width), rows.dtype),
            dma((2, nodes)), dma((2, nodes)),
            dma((2, 3, nodes)), dma((2, 3, nodes)),
            dma((2, 4 * nodes)), dma((2, 4 * nodes)),
            dma, dma((2 * devices,)),
        ],
        compiler_params=pltpu.CompilerParams(collective_id=0, has_side_effects=True),
        name="gather_tokens",
    )(rows)


def scatter_kernel(nodes, in_ref, out_ref, mine, r1, r2, r3, r4, s1, t1, s2, t2, s3, t3, s4, t4,
                   in_sem):
    p = Place(nodes)
    width = mine.shape[2]
    half = width // LANES // 2 * LANES
    cols = (pl.ds(0, half), pl.ds(half, width - half))
    loads = []
    order = list(range(1, nodes)) + [0]
    spots = {0: ((1, 1), (1, 0), (0, 1), (0, 0)), 1: ((1, 1), (0, 1), (1, 0), (0, 0))}
    sequence = [(h, k, s) for k in range(4) for s in order for h in range(2)]

    def at(h, k, s, c):
        fy, fx = spots[h][k]
        y = 1 - p.y if fy else p.y
        x = 1 - p.x if fx else p.x
        return p.block(p.other_z(s), y, x, c)

    for n, (h, k, s) in enumerate(sequence):
        for own in range(2):
            block = at(h, k, s, p.c if own else 1 - p.c)
            load = pltpu.make_async_copy(
                in_ref.at[block, :, cols[h]], mine.at[block, :, cols[h]], in_sem.at[own, n])
            load.start()
            loads.append(load)
    greet(p)
    sends = []

    def push(src, dst, send, recv, who):
        one = pltpu.make_async_remote_copy(src, dst, send, recv, device_id=who, device_id_type=MESH)
        one.start()
        sends.append(one)

    def arrive(dst, recv):
        pltpu.make_async_remote_copy(
            dst, dst, recv, recv, device_id=p.dev(c=1 - p.c), device_id_type=MESH).wait_recv()

    def plus(first, second):
        return first.astype(jnp.float32) + second.astype(jnp.float32)

    first_link = (p.dev(y=1 - p.y), p.dev(x=1 - p.x))
    second_link = (p.dev(x=1 - p.x), p.dev(y=1 - p.y))
    for n, (h, k, s) in enumerate(sequence):
        loads[2 * n].wait()
        push(mine.at[at(h, k, s, 1 - p.c), :, cols[h]], r1.at[h, k, s], s1.at[h, k, s],
             t1.at[h, k, s], p.dev(c=1 - p.c))
    for n, (h, k, s) in enumerate(sequence):
        loads[2 * n + 1].wait()
        arrive(r1.at[h, k, s], t1.at[h, k, s])
        r1[h, k, s] = plus(r1[h, k, s], mine[at(h, k, s, p.c), :, cols[h]]).astype(jnp.bfloat16)
        if k < 2:
            push(r1.at[h, k, s], r2.at[h, k, s], s2.at[h, k, s], t2.at[h, k, s], first_link[h])
    for s in order:
        for h in range(2):
            arrive(r2.at[h, 0, s], t2.at[h, 0, s])
            r2[h, 0, s] = plus(r2[h, 0, s], r1[h, 2, s]).astype(jnp.bfloat16)
            push(r2.at[h, 0, s], r3.at[h, s], s3.at[h, s], t3.at[h, s], second_link[h])
    for s in order:
        for h in range(2):
            arrive(r2.at[h, 1, s], t2.at[h, 1, s])
            arrive(r3.at[h, s], t3.at[h, s])
            total = plus(r2[h, 1, s], r1[h, 3, s]) + r3[h, s].astype(jnp.float32)
            r3[h, s] = total.astype(jnp.bfloat16)
            if s:
                push(r3.at[h, s], r4.at[h, s], s4.at[h, s], t4.at[h, s], p.dev(z=p.other_z(s)))
    for h in range(2):
        total = r3[h, 0].astype(jnp.float32)
        for s in range(1, nodes):
            arrive(r4.at[h, s], t4.at[h, s])
            total = total + r4[h, s].astype(jnp.float32)
        out_ref[:, cols[h]] = total.astype(jnp.bfloat16)
    for one in sends:
        one.wait_send()


def scatter_sums(terms, nodes):
    devices, count, width = terms.shape
    half = width // 2
    dma = pltpu.SemaphoreType.DMA
    vmem = lambda *lead: pltpu.VMEM((*lead, count, half), terms.dtype)
    return pl.pallas_call(
        lambda *refs: scatter_kernel(nodes, *refs),
        out_shape=jax.ShapeDtypeStruct((count, width), terms.dtype),
        in_specs=[pl.BlockSpec(memory_space=pl.ANY)],
        out_specs=pl.BlockSpec(memory_space=pltpu.VMEM),
        scratch_shapes=[
            pltpu.VMEM((devices, count, width), terms.dtype),
            vmem(2, 4, nodes), vmem(2, 2, nodes), vmem(2, nodes), vmem(2, nodes),
            dma((2, 4, nodes)), dma((2, 4, nodes)),
            dma((2, 2, nodes)), dma((2, 2, nodes)),
            dma((2, nodes)), dma((2, nodes)),
            dma((2, nodes)), dma((2, nodes)),
            dma((2, devices)),
        ],
        compiler_params=pltpu.CompilerParams(collective_id=1, has_side_effects=True),
        name="scatter_sums",
    )(terms)


def expert_kernel(nodes, slots, rows_ref, gate_ref, up_ref, down_ref, sgate_ref, sup_ref, sdown_ref,
                  out_ref, rows, gate, up, down, sgate, sup, sdown, out, weight, place_t, place,
                  picked, hidden, rows_sem, gate_sem, up_sem, down_sem, s_sem, sdown_sem, out_sem):
    total = rows.shape[0]
    width = down.shape[1]
    tile_d, tile_f = 512, 256
    steps_d, steps_f = width // tile_d, gate.shape[1] // tile_f
    experts = nodes * 8
    count = total // experts
    node = lax.axis_index("node")
    me = node * 8 + lax.axis_index("chip")
    group = pl.ds(pl.multiple_of(node * 8 * count, 8 * count), 8 * count)
    tail = pl.ds(width, rows.shape[1] - width)
    f32, bf16 = jnp.float32, jnp.bfloat16

    def cols(j, tile):
        return pl.ds(pl.multiple_of(j * tile, tile), tile)

    def part(src, dst, at, sem):
        return pltpu.make_async_copy(src.at[:, at], dst.at[:, at], sem)

    def rows_part(j):
        return part(rows_ref, rows, cols(j, tile_d), rows_sem.at[j])

    def gate_part(j):
        return part(gate_ref, gate, cols(j, tile_f), gate_sem.at[j])

    def up_part(j):
        return part(up_ref, up, cols(j, tile_f), up_sem.at[j])

    def down_part(j):
        return part(down_ref, down, cols(j, tile_d), down_sem.at[j])

    def sdown_part(j):
        return part(sdown_ref, sdown, cols(j, tile_d), sdown_sem.at[j])

    def out_part(j):
        return part(out, out_ref, cols(j, tile_d), out_sem.at[j])

    tail_copy = part(rows_ref, rows, tail, rows_sem.at[steps_d])
    sgate_copy = pltpu.make_async_copy(sgate_ref, sgate, s_sem.at[0])
    sup_copy = pltpu.make_async_copy(sup_ref, sup, s_sem.at[1])
    tail_copy.start()
    for j in range(steps_d):
        rows_part(j).start()
    for j in range(steps_f):
        gate_part(j).start()
        up_part(j).start()
    sgate_copy.start()
    sup_copy.start()
    for j in range(steps_d):
        down_part(j).start()
        sdown_part(j).start()

    def dot(first, second):
        return jnp.dot(first, second, preferred_element_type=f32)

    tail_copy.wait()
    side = rows[:, tail]
    lane = lax.broadcasted_iota(jnp.int32, (side.shape[1], LANES), 0)
    mine = (lane == me) | (lane == experts + me)
    weight[...] = dot(side, mine.astype(f32).astype(bf16))
    chosen = weight[...] > 0
    token = lax.broadcasted_iota(jnp.int32, (total, total), 0)
    other = lax.broadcasted_iota(jnp.int32, (total, total), 1)
    ahead = (token // count == other // count) & (other <= token)
    rank = dot(ahead.astype(f32).astype(bf16), chosen.astype(f32).astype(bf16))
    block = lax.broadcasted_iota(jnp.int32, (total, LANES), 0) // count
    slot = jnp.where(chosen, rank.astype(jnp.int32) - 1 + block * slots, -1)
    for k in range(experts * slots // LANES):
        spot = lax.broadcasted_iota(jnp.int32, (total, LANES), 1) + k * LANES
        hit = (slot == spot).astype(f32)
        place_t[:, k * LANES:(k + 1) * LANES] = hit.astype(bf16)
        place[k * LANES:(k + 1) * LANES, :] = hit.T.astype(bf16)

    @pl.loop(0, steps_d)
    def _(j):
        rows_part(j).wait()
        at = cols(j, tile_d)
        picked[:, at] = dot(place[...], rows[:, at]).astype(bf16)

    def glu(gate_sum, up_sum):
        return (jax.nn.silu(gate_sum) * up_sum).astype(bf16)

    @pl.loop(0, steps_f)
    def _(j):
        at = cols(j, tile_f)
        gate_part(j).wait()
        gate_sum = dot(picked[...], gate[:, at])
        up_part(j).wait()
        hidden[:, at] = glu(gate_sum, dot(picked[...], up[:, at]))

    sgate_copy.wait()
    sup_copy.wait()
    near = rows[group, 0:width]
    shared = glu(dot(near, sgate[...]), dot(near, sup[...]))

    @pl.loop(0, steps_d)
    def _(j):
        at = cols(j, tile_d)
        down_part(j).wait()
        result = dot(hidden[...], down[:, at]).astype(bf16)
        sdown_part(j).wait()
        partial = dot(shared, sdown[:, at])
        for r in range(nodes):
            span = slice(r * 8 * count, (r + 1) * 8 * count)
            terms = dot(place_t[span, :], result) * weight[span, 0:1]
            terms = terms + jnp.where(node == r, partial, 0.0)
            out[span, at] = terms.astype(bf16)
        out_part(j).start()

    for j in range(steps_d):
        out_part(j).wait()


def run_experts(rows, gate, up, down, sgate, sup, sdown, nodes, slots):
    total = rows.shape[0]
    width = down.shape[1]
    count = nodes * 8 * slots
    steps_d, steps_f = width // 512, gate.shape[1] // 256
    dma = pltpu.SemaphoreType.DMA
    bf16 = jnp.bfloat16
    hold = lambda a: pltpu.VMEM(a.shape, a.dtype)
    operands = (rows, gate, up, down, sgate, sup, sdown)
    return pl.pallas_call(
        lambda *refs: expert_kernel(nodes, slots, *refs),
        out_shape=jax.ShapeDtypeStruct((total, width), bf16),
        in_specs=[pl.BlockSpec(memory_space=pl.ANY)] * len(operands),
        out_specs=pl.BlockSpec(memory_space=pl.ANY),
        scratch_shapes=[hold(a) for a in operands] + [
            pltpu.VMEM((total, width), bf16),
            pltpu.VMEM((total, LANES), jnp.float32),
            pltpu.VMEM((total, count), bf16),
            pltpu.VMEM((count, total), bf16),
            pltpu.VMEM((count, width), bf16),
            pltpu.VMEM((count, gate.shape[1]), bf16),
            dma((steps_d + 1,)), dma((steps_f,)), dma((steps_f,)), dma((steps_d,)),
            dma((2,)), dma((steps_d,)), dma((steps_d,)),
        ],
        compiler_params=pltpu.CompilerParams(vmem_limit_bytes=60 * 2**20),
        name="run_experts",
    )(*operands)


def local(
    tokens,
    expert_ids,
    route_weight,
    expert_gate,
    expert_up,
    expert_down,
    shared_gate,
    shared_up,
    shared_down,
    query_latent,
    query_rope,
    cache_latent,
    cache_rope,
    cache_len,
):
    node_count = lax.axis_size("node")
    chip_count = lax.axis_size("chip")
    experts = node_count * chip_count
    tok_rows, model_width = tokens.shape
    top = expert_ids.shape[1]
    slots = (2 * tok_rows * top + experts - 1) // experts
    trees = chip_count == 8
    node, chip = lax.axis_index("node"), lax.axis_index("chip")
    me = node * chip_count + chip

    names = jnp.arange(experts, dtype=jnp.int32)
    dense = jnp.sum(
        jnp.where(expert_ids[:, :, None] == names, route_weight[:, :, None], 0.0), axis=1
    )
    high = lax.reduce_precision(dense, 8, 7)
    low = dense - high
    side = jnp.concatenate([high, low], axis=1).astype(jnp.bfloat16)
    side = jnp.pad(side, ((0, 0), (0, -(2 * experts) % LANES)))
    rows = jnp.concatenate([tokens, side], axis=1)
    if trees:
        gathered = gather_tokens(rows, node_count)
    else:
        gathered = lax.all_gather(rows, ("node", "chip"), axis=0)
    total = experts * tok_rows
    if trees:
        terms = run_experts(
            gathered.reshape(total, -1), expert_gate[0], expert_up[0], expert_down[0],
            shared_gate, shared_up, shared_down, node_count, slots,
        )
        moe_out = scatter_sums(terms.reshape(experts, tok_rows, model_width), node_count)
        return moe_out, attend(query_latent, query_rope, cache_latent, cache_rope, cache_len)
    flat = gathered.reshape(total, -1)
    every = flat[:, :model_width]
    tail = flat[:, model_width:].astype(jnp.float32)
    lane = lax.broadcasted_iota(jnp.int32, (1, tail.shape[1]), 1)
    scale = jnp.sum(jnp.where((lane == me) | (lane == experts + me), tail, 0.0), axis=1)

    chosen = (scale > 0).reshape(experts, tok_rows)
    rank = jnp.cumsum(chosen.astype(jnp.int32), axis=1) - 1
    slot = jnp.where(chosen, rank + slots * names[:, None], -1).reshape(-1)
    place = (jnp.arange(experts * slots, dtype=jnp.int32)[:, None] == slot[None, :])
    place = place.astype(jnp.bfloat16)
    picked = jnp.dot(place, every, preferred_element_type=jnp.float32).astype(jnp.bfloat16)
    hidden = swiglu_hidden(picked, expert_gate[0], expert_up[0])
    result = jnp.dot(hidden, expert_down[0], preferred_element_type=jnp.float32)
    result = result.astype(jnp.bfloat16)
    spread = lax.dot_general(
        place, result, (((0,), (0,)), ((), ())), preferred_element_type=jnp.float32
    )
    group = lax.dynamic_slice_in_dim(every, node * chip_count * tok_rows, chip_count * tok_rows, 0)
    shared_hidden = swiglu_hidden(group, shared_gate, shared_up)
    partial_terms = jnp.dot(shared_hidden, shared_down, preferred_element_type=jnp.float32)
    terms = (spread * scale[:, None]).reshape(node_count, -1, model_width)
    own_node = jnp.arange(node_count) == node
    terms = terms + jnp.where(own_node[:, None, None], partial_terms[None], 0.0)
    terms = terms.astype(jnp.bfloat16).reshape(experts, tok_rows, model_width)
    moe_out = lax.psum_scatter(
        terms.reshape(total, model_width), ("node", "chip"), scatter_dimension=0, tiled=True
    )
    attn_out = attend(query_latent, query_rope, cache_latent, cache_rope, cache_len)
    return (moe_out, attn_out)


def solution(mesh):
    placed = (
        P(("node", "chip"), None),
        P(("node", "chip"), None),
        P(("node", "chip"), None),
        P(("node", "chip"), None, None),
        P(("node", "chip"), None, None),
        P(("node", "chip"), None, None),
        P(None, "chip"),
        P(None, "chip"),
        P("chip", None),
        P(("node", "chip"), None, None),
        P(("node", "chip"), None),
        P(("node", "chip"), None, None),
        P(("node", "chip"), None, None),
        P(("node", "chip")),
    )
    return jax.shard_map(
        local,
        mesh=mesh,
        in_specs=placed,
        out_specs=(P(("node", "chip"), None), P(("node", "chip"), None, None)),
        check_vma=False,
    )
```
